32 devices in a mesh: chan: 2 (over x), vis: 2 (over core), pix: 8 (over z, y).
Axes of the slice: x: 2, y: 2, z: 4, core: 2. Of those that a mesh axis runs over, the one named last changes fastest.
Arguments:
- response: bfloat16 [16384, 49152], P(('chan', 'vis'), 'pix'), parts along dimension 0, may hold values from -5 to 5
- vis_data: float32 [16384], P(('chan', 'vis')), parts along dimension 0, may hold values from -6 to 6
- baseline_of_row: int32 [8192], P('vis'), may hold values from 0 to 8191
- noise_class: int32 [8192], P('vis'), may hold values from 0 to 15
- baseline_weight: float32 [8192], replicated, may hold values from 0.25 to 4
- class_inv_var: float32 [32], P('chan'), parts along dimension 0, may hold values from 0.25 to 4
Outputs:
- sky_map: float32 [98304], P(('chan', 'pix')), parts along dimension 0
- psf: float32 [98304, 64], P(('chan', 'pix'), 'vis'), parts along dimension 0
The draws below stay inside these ranges and needn't reach their ends.
There are 2 independent parts, one for each index of `chan`. The reference program is written for one: setup_inputs(seed, part) draws one part's arguments, and reference() takes and returns one part's arrays. A program takes and returns all parts, laid end to end along the dimension named above; an argument that names none is the same for every part. Nothing has to cross between parts.
Inputs may be any that keep to these rules, and one draw needn't show every extreme that they name: `baseline_of_row`: baseline index of each row.
All inputs are finite; a program needn't handle non-finite values.
Results may differ from the reference program's by a relative error of at most 0.0041.
Values may be sent and summed in bfloat16 or wider, within the bound.
A program may use at most 128 MiB of HBM per device.

```python
import math
import jax
import jax.numpy as jnp
from jax import lax

PIX = 49152
PANEL_DEV = 8
NBL = 8192
NCLASS = 16
VIS = 8192
N_PIX = 8


def with_ends(entries, stream_key, smallest, largest):
    place = [jax.random.randint(jax.random.fold_in(stream_key, axis), (), 0, length) for axis, length in enumerate(entries.shape)]
    longest = entries.shape.index(max(entries.shape))
    beside = place[:longest] + [(place[longest] + 1) % entries.shape[longest]] + place[longest + 1:]
    return entries.at[tuple(place)].set(smallest).at[tuple(beside)].set(largest)


def steps_of(own_key, dims, shards, least, top_value):
    def one(axis_at, parts):
        draws = jax.random.uniform(jax.random.fold_in(jax.random.fold_in(own_key, 6), axis_at), (parts,), jnp.float32, least / len(shards), top_value / len(shards))
        return jnp.repeat(jnp.exp(draws), dims[axis_at] // parts).reshape((-1,) + (1,) * (len(dims) - axis_at - 1))

    gain = one(*shards[0])
    for cut in shards[1:]:
        gain = gain * one(*cut)
    return gain


def noise(key, extent, spread, limit, cuts=(), held_as=jnp.bfloat16):
    loudness = steps_of(key, extent, cuts, -0.22, 0.18) if cuts else 1.0
    result = jax.random.normal(key, extent, jnp.float32) * spread * loudness
    return jnp.minimum(jnp.maximum(result, -limit), limit).astype(held_as)


def setup_inputs(seed: int = 0, part: int = 0) -> dict:
    seeds = jax.random.split(jax.random.key(seed), 7)
    part_keys = jax.random.split(jax.random.fold_in(seeds[6], part), 7)
    return {
        "response": noise(part_keys[0], (VIS, PIX), 1.0, 5.0, ((0, 2), (1, 8))),
        "vis_data": noise(part_keys[1], (VIS,), 1.0, 6.0, ((0, 2),), jnp.float32),
        "baseline_of_row": with_ends(jax.random.randint(seeds[2], (VIS,), 0, NBL), jax.random.fold_in(seeds[2], 1), 0, NBL - 1).astype(jnp.int32),
        "noise_class": with_ends(jax.random.randint(seeds[3], (VIS,), 0, NCLASS), jax.random.fold_in(seeds[3], 1), 0, NCLASS - 1).astype(jnp.int32),
        "baseline_weight": jnp.clip(jnp.exp(jax.random.uniform(seeds[4], (NBL,), jnp.float32, math.log(0.25), math.log(4.0))), 0.25, 4.0),
        "class_inv_var": jnp.clip(jnp.exp(jax.random.uniform(part_keys[5], (NCLASS,), jnp.float32, math.log(0.25), math.log(4.0))), 0.25, 4.0),
    }


def add_norm(total, pair):
    resp_block, weight_block = pair
    squares = jnp.square(resp_block.astype(jnp.float32))
    return (total + lax.optimization_barrier(jnp.sum(weight_block[:, None] * squares, axis=0)), None)

def reference(response, vis_data, baseline_of_row, noise_class, baseline_weight, class_inv_var):
    weight_row = baseline_weight[baseline_of_row] * class_inv_var[noise_class]
    pix_block = PIX // N_PIX
    blocks = response.reshape(VIS, N_PIX, pix_block)
    panel_cols = blocks[:, :, :PANEL_DEV].reshape(VIS, N_PIX * PANEL_DEV)
    weighted_panel = (weight_row[:, None] * panel_cols.astype(jnp.float32)).astype(jnp.bfloat16)
    weighted_vis = (weight_row * vis_data).astype(jnp.bfloat16)
    dirty_map = jnp.dot(weighted_vis, response, preferred_element_type=jnp.float32)
    row_step = math.gcd(VIS, 512)
    stacked = response.reshape(VIS // row_step, row_step, PIX)
    stacked_weight = weight_row.reshape(VIS // row_step, row_step)
    pixel_norm, unused = lax.scan(add_norm, jnp.zeros((PIX,), jnp.float32), (stacked, stacked_weight))
    beam_full = jnp.dot(response.T, weighted_panel, preferred_element_type=jnp.float32)
    panel_norm = pixel_norm.reshape(N_PIX, pix_block)[:, :PANEL_DEV].reshape(N_PIX * PANEL_DEV)
    sky_map = dirty_map / jnp.sqrt(pixel_norm)
    psf = beam_full / jnp.sqrt(pixel_norm[:, None] * panel_norm[None, :])
    return (sky_map, psf)
```

```python
import functools

import jax
import jax.numpy as jnp
from jax import lax
from jax.experimental import pallas as pl
from jax.experimental.pallas import tpu as pltpu
from jax.sharding import PartitionSpec as P

PANEL_DEV = 8
LANES = 128
EXTRA = 16
MESH_ID = pl.DeviceIdType.MESH
F32, BF16 = jnp.float32, jnp.bfloat16


def kernel(
    n_pix, n_early,
    resp, vis_h, base_h, cls_h, bw_h, civ_h,
    sky_h, psf_h,
    x, vis, base, cls, bw, civ, pbuf, w_ref, w2, lhs, nbuf, keep, sbuf, rbuf,
    qpart, qown, qrecv, psf, sky,
    in_sem, small_sem, psend, precv, vsend, vrecv, qsem, out_sem,
):
    n_chunk, rows, ch = x.shape
    n_panel = n_pix * PANEL_DEV
    half = n_panel // 2
    me = lax.axis_index("pix")
    v = lax.axis_index("vis")
    other = 1 - v

    first = pltpu.make_async_copy(
        resp.at[:, pl.ds(0, LANES)], x.at[0, :, pl.ds(0, LANES)], in_sem.at[n_chunk]
    )
    first.start()
    smalls = [
        pltpu.make_async_copy(a, b, small_sem.at[i])
        for i, (a, b) in enumerate(
            [(vis_h, vis), (base_h, base), (cls_h, cls), (bw_h, bw), (civ_h, civ)]
        )
    ]
    for c in smalls:
        c.start()
    rest = None
    if ch > LANES:
        rest = pltpu.make_async_copy(
            resp.at[:, pl.ds(LANES, ch - LANES)],
            x.at[0, :, pl.ds(LANES, ch - LANES)],
            in_sem.at[0],
        )
        rest.start()

    def chunk_copy(c):
        return pltpu.make_async_copy(
            resp.at[:, pl.ds(pl.multiple_of(c * ch, ch), ch)], x.at[c], in_sem.at[c]
        )

    for c in range(1, n_chunk):
        chunk_copy(c).start()

    barrier = pltpu.get_barrier_semaphore()

    def greet(d, carry):
        pl.semaphore_signal(
            barrier, inc=1, device_id={"pix": lax.rem(me + d, n_pix)}, device_id_type=MESH_ID
        )
        return carry

    lax.fori_loop(1, n_pix, greet, 0)
    pl.semaphore_signal(barrier, inc=1, device_id={"vis": other}, device_id_type=MESH_ID)

    first.wait()
    pick = (
        lax.broadcasted_iota(jnp.int32, (16, LANES), 0)
        == lax.broadcasted_iota(jnp.int32, (16, LANES), 1)
    ).astype(BF16)
    own = lax.dot_general(
        pick, x[0, :, :LANES], (((1,), (1,)), ((), ())), preferred_element_type=F32
    )
    pbuf[me] = own[:PANEL_DEV].astype(BF16)
    pl.semaphore_wait(barrier, n_pix)

    def panel_copy(slot, peer):
        return pltpu.make_async_remote_copy(
            src_ref=pbuf.at[slot], dst_ref=pbuf.at[slot],
            send_sem=psend.at[peer], recv_sem=precv.at[slot],
            device_id={"pix": peer}, device_id_type=MESH_ID,
        )

    def send_panel(d, carry):
        panel_copy(me, lax.rem(me + d, n_pix)).start()
        return carry

    lax.fori_loop(1, n_pix, send_panel, 0)

    for c in smalls:
        c.wait()
    n_hi = bw.shape[0]
    t0 = bw[...].astype(BF16)
    left = bw[...] - t0.astype(F32)
    t1 = left.astype(BF16)
    t2 = (left - t1.astype(F32)).astype(BF16)
    table = jnp.concatenate([t0, t1, t2], axis=0)
    n_cls = civ.shape[1]
    diag = lax.broadcasted_iota(jnp.int32, (n_cls, n_cls), 0) == lax.broadcasted_iota(
        jnp.int32, (n_cls, n_cls), 1
    )
    civ_col = jnp.sum(
        jnp.where(diag, jnp.broadcast_to(civ[...], (n_cls, n_cls)), 0.0), axis=1, keepdims=True
    )
    step = min(rows, 512)

    def weights(i, carry):
        cols = pl.ds(pl.multiple_of(i * step, step), step)
        idx = base[:, cols]
        hi = lax.broadcast_in_dim(idx // LANES, (n_hi, step), (0, 1))
        lo = lax.broadcast_in_dim(lax.rem(idx, LANES), (LANES, step), (0, 1))
        hot = (hi == lax.broadcasted_iota(jnp.int32, (n_hi, step), 0)).astype(F32).astype(BF16)
        picked = lax.dot_general(
            table, jnp.concatenate([hot] * 3, axis=0), (((0,), (0,)), ((), ())),
            preferred_element_type=F32,
        )
        bw_row = jnp.sum(
            jnp.where(lo == lax.broadcasted_iota(jnp.int32, (LANES, step), 0), picked, 0.0),
            axis=0, keepdims=True,
        )
        kinds = lax.broadcast_in_dim(cls[:, cols], (n_cls, step), (0, 1))
        cw_row = jnp.sum(
            jnp.where(
                kinds == lax.broadcasted_iota(jnp.int32, (n_cls, step), 0), civ_col, 0.0
            ),
            axis=0, keepdims=True,
        )
        w = bw_row * cw_row
        w_ref[:, cols] = w
        w_hi = w.astype(BF16).astype(F32)
        at = lax.broadcasted_iota(jnp.int32, (EXTRA, step), 0)
        w2[:, cols] = jnp.where(
            at == 0, w_hi, jnp.where(at == 1, w - w_hi, 0.0)
        ).astype(BF16)
        lhs[n_panel:, cols] = jnp.where(at == 0, w * vis[:, cols], 0.0).astype(BF16)
        return carry

    lax.fori_loop(0, rows // step, weights, 0)

    kb = min(rows, 512)

    def norm_of(c):
        acc = None
        for k in range(0, rows, kb):
            xb = x[c, k : k + kb, :]
            part = jnp.dot(w2[:, k : k + kb], xb * xb, preferred_element_type=F32)
            acc = part if acc is None else acc + part
        nbuf[c] = jnp.broadcast_to(jnp.sum(acc, axis=0, keepdims=True), (8, ch))

    def vis_copy(c):
        return pltpu.make_async_remote_copy(
            src_ref=sbuf.at[c], dst_ref=rbuf.at[c],
            send_sem=vsend.at[c], recv_sem=vrecv.at[c],
            device_id={"vis": other}, device_id_type=MESH_ID,
        )

    def beam_of(c):
        res = jnp.dot(lhs[...], x[c], preferred_element_type=F32)
        at = lax.broadcasted_iota(jnp.int32, (8, ch), 0)
        pair = jnp.where(
            at == 0, res[n_panel : n_panel + 8], jnp.where(at == 1, nbuf[c], 0.0)
        )
        keep[c, :half] = res[:half]
        keep[c, half:] = pair
        sbuf[c, :half] = res[half:n_panel]
        sbuf[c, half:] = pair
        vis_copy(c).start()

    if rest is not None:
        rest.wait()
    norm_of(0)

    def early(c, carry):
        chunk_copy(c).wait()
        norm_of(c)
        return carry

    lax.fori_loop(1, n_early, early, 0)

    def wait_panel(d, carry):
        slot = lax.rem(me + d, n_pix)
        panel_copy(slot, slot).wait_recv()
        return carry

    lax.fori_loop(1, n_pix, wait_panel, 0)

    def weigh(j, carry):
        w = w_ref[...]
        src = lax.rem(2 * j + v * (n_pix // 2), n_pix)
        a = pbuf[src].astype(F32)
        b = pbuf[src + 1].astype(F32)
        wa, wb = w * a, w * b
        lhs[pl.ds(pl.multiple_of(j * 16, 16), 16), :] = jnp.concatenate([wa, wb], axis=0).astype(
            BF16
        )
        sq = jnp.concatenate(
            [
                jnp.sum(wa * a, axis=1, keepdims=True),
                jnp.sum(wb * b, axis=1, keepdims=True),
            ],
            axis=0,
        )
        qpart[pl.ds(pl.multiple_of(j * 16, 16), 16), :] = jnp.broadcast_to(sq, (16, LANES))
        return carry

    lax.fori_loop(0, n_pix // 2, weigh, 0)
    q_copy = pltpu.make_async_remote_copy(
        src_ref=qpart.at[pl.ds(half, half)], dst_ref=qrecv,
        send_sem=qsem.at[0], recv_sem=qsem.at[1],
        device_id={"vis": other}, device_id_type=MESH_ID,
    )
    q_copy.start()

    def backlog(c, carry):
        beam_of(c)
        return carry

    lax.fori_loop(0, n_early, backlog, 0)

    def late(c, carry):
        chunk_copy(c).wait()
        norm_of(c)
        beam_of(c)
        return carry

    lax.fori_loop(n_early, n_chunk, late, 0)

    q_copy.wait()
    qown[...] = lax.rsqrt(qpart[:half, :1] + qrecv[:, :1]) * jnp.ones((1, LANES), F32)

    def out_copies(c):
        cols = pl.ds(pl.multiple_of(c * ch, ch), ch)
        return (
            pltpu.make_async_copy(psf.at[c], psf_h.at[:, cols], out_sem.at[0, c]),
            pltpu.make_async_copy(sky.at[c], sky_h.at[:, cols], out_sem.at[1, c]),
        )

    def final(c, carry):
        vis_copy(c).wait_recv()
        pair = keep[c, half:] + rbuf[c, half:]
        scale = lax.rsqrt(pair[1:2])
        sky[c] = pair[0:1] * scale
        psf[c] = (keep[c, :half] + rbuf[c, :half]) * scale * qown[:, :1]
        for o in out_copies(c):
            o.start()
        return carry

    lax.fori_loop(0, n_chunk, final, 0)

    def drain(c, carry):
        vis_copy(c).wait_send()
        for o in out_copies(c):
            o.wait()
        return carry

    lax.fori_loop(0, n_chunk, drain, 0)

    def drain_panel(d, carry):
        panel_copy(me, lax.rem(me + d, n_pix)).wait_send()
        return carry

    lax.fori_loop(1, n_pix, drain_panel, 0)


def shards(n_pix, response, vis_data, baseline_of_row, noise_class, baseline_weight, class_inv_var):
    rows, pix = response.shape
    ch = next(c for c in (512, 256, 128) if pix % c == 0)
    n_chunk = pix // ch
    n_early = max(1, n_chunk // 2)
    n_panel = n_pix * PANEL_DEV
    half = n_panel // 2
    n_hi = baseline_weight.shape[0] // LANES
    n_cls = class_inv_var.shape[0]
    vmem, dma = pltpu.VMEM, pltpu.SemaphoreType.DMA
    any_space = pl.BlockSpec(memory_space=pl.ANY)
    sky, psf = pl.pallas_call(
        functools.partial(kernel, n_pix, n_early),
        out_shape=(
            jax.ShapeDtypeStruct((1, pix), F32),
            jax.ShapeDtypeStruct((half, pix), F32),
        ),
        in_specs=[any_space] * 6,
        out_specs=(any_space, any_space),
        scratch_shapes=[
            vmem((n_chunk, rows, ch), BF16),
            vmem((1, rows), F32),
            vmem((1, rows), jnp.int32),
            vmem((1, rows), jnp.int32),
            vmem((n_hi, LANES), F32),
            vmem((1, n_cls), F32),
            vmem((n_pix, PANEL_DEV, rows), BF16),
            vmem((1, rows), F32),
            vmem((EXTRA, rows), BF16),
            vmem((n_panel + EXTRA, rows), BF16),
            vmem((n_chunk, 8, ch), F32),
            vmem((n_chunk, half + 8, ch), F32),
            vmem((n_chunk, half + 8, ch), F32),
            vmem((n_chunk, half + 8, ch), F32),
            vmem((n_panel, LANES), F32),
            vmem((half, LANES), F32),
            vmem((half, LANES), F32),
            vmem((n_chunk, half, ch), F32),
            vmem((n_chunk, 1, ch), F32),
            dma((n_chunk + 1,)),
            dma((5,)),
            dma((n_pix,)),
            dma((n_pix,)),
            dma((n_chunk,)),
            dma((n_chunk,)),
            dma((2,)),
            dma((2, n_chunk)),
        ],
        compiler_params=pltpu.CompilerParams(
            collective_id=0, has_side_effects=True, vmem_limit_bytes=63 * 1024 * 1024
        ),
    )(
        response,
        vis_data.reshape(1, rows),
        baseline_of_row.reshape(1, rows),
        noise_class.reshape(1, rows),
        baseline_weight.reshape(n_hi, LANES),
        class_inv_var.reshape(1, n_cls),
    )
    return sky.reshape(pix), psf.T


def solution(mesh):
    placed = (P(("chan", "vis"), "pix"), P(("chan", "vis")), P("vis"), P("vis"), P(), P("chan"))
    return jax.shard_map(
        functools.partial(shards, mesh.shape["pix"]),
        mesh=mesh,
        in_specs=placed,
        out_specs=(P(("chan", "pix")), P(("chan", "pix"), "vis")),
        check_vma=False,
    )
```

```python
import functools

import jax
import jax.numpy as jnp
from jax import lax
from jax.experimental import pallas as pl
from jax.experimental.pallas import tpu as pltpu
from jax.sharding import PartitionSpec as P

PANEL_DEV = 8
LANES = 128
EXTRA = 16
MESH_ID = pl.DeviceIdType.MESH
F32, BF16 = jnp.float32, jnp.bfloat16


def kernel(
    n_pix, n_early,
    resp, vis_h, base_h, cls_h, bw_h, civ_h,
    sky, psf,
    x, vis, base, cls, bw, civ, pbuf, w_ref, w2, lhs, nbuf, keep, sbuf, rbuf,
    qpart, qown, qrecv,
    in_sem, small_sem, psend, precv, vsend, vrecv, qsem,
):
    n_chunk, rows, ch = x.shape
    n_panel = n_pix * PANEL_DEV
    half = n_panel // 2
    me = lax.axis_index("pix")
    v = lax.axis_index("vis")
    other = 1 - v

    first = pltpu.make_async_copy(
        resp.at[:, pl.ds(0, LANES)], x.at[0, :, pl.ds(0, LANES)], in_sem.at[n_chunk]
    )
    first.start()
    smalls = [
        pltpu.make_async_copy(a, b, small_sem.at[i])
        for i, (a, b) in enumerate(
            [(vis_h, vis), (base_h, base), (cls_h, cls), (bw_h, bw), (civ_h, civ)]
        )
    ]
    for c in smalls:
        c.start()
    rest = None
    if ch > LANES:
        rest = pltpu.make_async_copy(
            resp.at[:, pl.ds(LANES, ch - LANES)],
            x.at[0, :, pl.ds(LANES, ch - LANES)],
            in_sem.at[0],
        )
        rest.start()

    def chunk_copy(c):
        return pltpu.make_async_copy(
            resp.at[:, pl.ds(pl.multiple_of(c * ch, ch), ch)], x.at[c], in_sem.at[c]
        )

    for c in range(1, n_chunk):
        chunk_copy(c).start()

    barrier = pltpu.get_barrier_semaphore()

    def greet(d, carry):
        pl.semaphore_signal(
            barrier, inc=1, device_id={"pix": lax.rem(me + d, n_pix)}, device_id_type=MESH_ID
        )
        return carry

    lax.fori_loop(1, n_pix, greet, 0)
    pl.semaphore_signal(barrier, inc=1, device_id={"vis": other}, device_id_type=MESH_ID)

    first.wait()
    pick = (
        lax.broadcasted_iota(jnp.int32, (16, LANES), 0)
        == lax.broadcasted_iota(jnp.int32, (16, LANES), 1)
    ).astype(BF16)
    own = lax.dot_general(
        pick, x[0, :, :LANES], (((1,), (1,)), ((), ())), preferred_element_type=F32
    )
    pbuf[me] = own[:PANEL_DEV].astype(BF16)
    pl.semaphore_wait(barrier, n_pix)

    def panel_copy(slot, peer):
        return pltpu.make_async_remote_copy(
            src_ref=pbuf.at[slot], dst_ref=pbuf.at[slot],
            send_sem=psend.at[peer], recv_sem=precv.at[slot],
            device_id={"pix": peer}, device_id_type=MESH_ID,
        )

    def send_panel(d, carry):
        panel_copy(me, lax.rem(me + d, n_pix)).start()
        return carry

    lax.fori_loop(1, n_pix, send_panel, 0)

    for c in smalls:
        c.wait()
    n_hi = bw.shape[0]
    t0 = bw[...].astype(BF16)
    left = bw[...] - t0.astype(F32)
    t1 = left.astype(BF16)
    t2 = (left - t1.astype(F32)).astype(BF16)
    table = jnp.concatenate([t0, t1, t2], axis=0)
    n_cls = civ.shape[1]
    diag = lax.broadcasted_iota(jnp.int32, (n_cls, n_cls), 0) == lax.broadcasted_iota(
        jnp.int32, (n_cls, n_cls), 1
    )
    civ_col = jnp.sum(
        jnp.where(diag, jnp.broadcast_to(civ[...], (n_cls, n_cls)), 0.0), axis=1, keepdims=True
    )
    step = min(rows, 512)

    def weights(i, carry):
        cols = pl.ds(pl.multiple_of(i * step, step), step)
        idx = base[:, cols]
        hi = lax.broadcast_in_dim(idx // LANES, (n_hi, step), (0, 1))
        lo = lax.broadcast_in_dim(lax.rem(idx, LANES), (LANES, step), (0, 1))
        hot = (hi == lax.broadcasted_iota(jnp.int32, (n_hi, step), 0)).astype(F32).astype(BF16)
        picked = lax.dot_general(
            table, jnp.concatenate([hot] * 3, axis=0), (((0,), (0,)), ((), ())),
            preferred_element_type=F32,
        )
        bw_row = jnp.sum(
            jnp.where(lo == lax.broadcasted_iota(jnp.int32, (LANES, step), 0), picked, 0.0),
            axis=0, keepdims=True,
        )
        kinds = lax.broadcast_in_dim(cls[:, cols], (n_cls, step), (0, 1))
        cw_row = jnp.sum(
            jnp.where(
                kinds == lax.broadcasted_iota(jnp.int32, (n_cls, step), 0), civ_col, 0.0
            ),
            axis=0, keepdims=True,
        )
        w = bw_row * cw_row
        w_ref[:, cols] = w
        w_hi = w.astype(BF16).astype(F32)
        at = lax.broadcasted_iota(jnp.int32, (EXTRA, step), 0)
        w2[:, cols] = jnp.where(
            at == 0, w_hi, jnp.where(at == 1, w - w_hi, 0.0)
        ).astype(BF16)
        lhs[n_panel:, cols] = jnp.where(at == 0, w * vis[:, cols], 0.0).astype(BF16)
        return carry

    lax.fori_loop(0, rows // step, weights, 0)

    kb = min(rows, 512)

    def norm_of(c):
        acc = None
        for k in range(0, rows, kb):
            xb = x[c, k : k + kb, :]
            part = jnp.dot(w2[:, k : k + kb], xb * xb, preferred_element_type=F32)
            acc = part if acc is None else acc + part
        nbuf[c] = jnp.broadcast_to(jnp.sum(acc, axis=0, keepdims=True), (8, ch))

    def vis_copy(c):
        return pltpu.make_async_remote_copy(
            src_ref=sbuf.at[c], dst_ref=rbuf.at[c],
            send_sem=vsend.at[c], recv_sem=vrecv.at[c],
            device_id={"vis": other}, device_id_type=MESH_ID,
        )

    def beam_of(c):
        res = jnp.dot(lhs[...], x[c], preferred_element_type=F32)
        at = lax.broadcasted_iota(jnp.int32, (8, ch), 0)
        pair = jnp.where(
            at == 0, res[n_panel : n_panel + 8], jnp.where(at == 1, nbuf[c], 0.0)
        )
        keep[c, :half] = res[:half]
        keep[c, half:] = pair
        sbuf[c, :half] = res[half:n_panel]
        sbuf[c, half:] = pair
        vis_copy(c).start()

    if rest is not None:
        rest.wait()
    norm_of(0)

    def early(c, carry):
        chunk_copy(c).wait()
        norm_of(c)
        return carry

    lax.fori_loop(1, n_early, early, 0)

    def wait_panel(d, carry):
        slot = lax.rem(me + d, n_pix)
        panel_copy(slot, slot).wait_recv()
        return carry

    lax.fori_loop(1, n_pix, wait_panel, 0)

    def weigh(j, carry):
        w = w_ref[...]
        src = lax.rem(2 * j + v * (n_pix // 2), n_pix)
        a = pbuf[src].astype(F32)
        b = pbuf[src + 1].astype(F32)
        wa, wb = w * a, w * b
        lhs[pl.ds(pl.multiple_of(j * 16, 16), 16), :] = jnp.concatenate([wa, wb], axis=0).astype(
            BF16
        )
        sq = jnp.concatenate(
            [
                jnp.sum(wa * a, axis=1, keepdims=True),
                jnp.sum(wb * b, axis=1, keepdims=True),
            ],
            axis=0,
        )
        qpart[pl.ds(pl.multiple_of(j * 16, 16), 16), :] = jnp.broadcast_to(sq, (16, LANES))
        return carry

    lax.fori_loop(0, n_pix // 2, weigh, 0)
    q_copy = pltpu.make_async_remote_copy(
        src_ref=qpart.at[pl.ds(half, half)], dst_ref=qrecv,
        send_sem=qsem.at[0], recv_sem=qsem.at[1],
        device_id={"vis": other}, device_id_type=MESH_ID,
    )
    q_copy.start()

    def backlog(c, carry):
        beam_of(c)
        return carry

    lax.fori_loop(0, n_early, backlog, 0)

    q_copy.wait()
    qown[...] = lax.rsqrt(qpart[:half, :1] + qrecv[:, :1]) * jnp.ones((1, LANES), F32)

    def final(c, carry):
        vis_copy(c).wait_recv()
        cols = pl.ds(pl.multiple_of(c * ch, ch), ch)
        pair = keep[c, half:] + rbuf[c, half:]
        scale = lax.rsqrt(pair[1:2])
        sky[:, cols] = pair[0:1] * scale
        psf[:, cols] = (keep[c, :half] + rbuf[c, :half]) * scale * qown[:, :1]
        return carry

    lax.fori_loop(0, n_early, final, 0)

    def late(c, carry):
        chunk_copy(c).wait()
        norm_of(c)
        beam_of(c)

        @pl.when(c > n_early)
        def _():
            final(c - 1, 0)

        return carry

    lax.fori_loop(n_early, n_chunk, late, 0)
    final(n_chunk - 1, 0)

    def drain(c, carry):
        vis_copy(c).wait_send()
        return carry

    lax.fori_loop(0, n_chunk, drain, 0)

    def drain_panel(d, carry):
        panel_copy(me, lax.rem(me + d, n_pix)).wait_send()
        return carry

    lax.fori_loop(1, n_pix, drain_panel, 0)


def shards(n_pix, response, vis_data, baseline_of_row, noise_class, baseline_weight, class_inv_var):
    rows, pix = response.shape
    ch = next(c for c in (1024, 768, 512, 256, 128) if pix % c == 0)
    n_chunk = pix // ch
    n_early = max(1, n_chunk // 3)
    n_panel = n_pix * PANEL_DEV
    half = n_panel // 2
    n_hi = baseline_weight.shape[0] // LANES
    n_cls = class_inv_var.shape[0]
    vmem, dma = pltpu.VMEM, pltpu.SemaphoreType.DMA
    sky, psf = pl.pallas_call(
        functools.partial(kernel, n_pix, n_early),
        out_shape=(
            pltpu.VMEM((1, pix), F32),
            pltpu.VMEM((half, pix), F32),
        ),
        in_specs=[pl.BlockSpec(memory_space=pltpu.HBM)] * 6,
        out_specs=(pl.BlockSpec(memory_space=pltpu.VMEM),) * 2,
        scratch_shapes=[
            vmem((n_chunk, rows, ch), BF16),
            vmem((1, rows), F32),
            vmem((1, rows), jnp.int32),
            vmem((1, rows), jnp.int32),
            vmem((n_hi, LANES), F32),
            vmem((1, n_cls), F32),
            vmem((n_pix, PANEL_DEV, rows), BF16),
            vmem((1, rows), F32),
            vmem((EXTRA, rows), BF16),
            vmem((n_panel + EXTRA, rows), BF16),
            vmem((n_chunk, 8, ch), F32),
            vmem((n_chunk, half + 8, ch), F32),
            vmem((n_chunk, half + 8, ch), F32),
            vmem((n_chunk, half + 8, ch), F32),
            vmem((n_panel, LANES), F32),
            vmem((half, LANES), F32),
            vmem((half, LANES), F32),
            dma((n_chunk + 1,)),
            dma((5,)),
            dma((n_pix,)),
            dma((n_pix,)),
            dma((n_chunk,)),
            dma((n_chunk,)),
            dma((2,)),
        ],
        compiler_params=pltpu.CompilerParams(
            collective_id=0, has_side_effects=True, vmem_limit_bytes=58 * 1024 * 1024
        ),
    )(
        response,
        vis_data.reshape(1, rows),
        baseline_of_row.reshape(1, rows),
        noise_class.reshape(1, rows),
        baseline_weight.reshape(n_hi, LANES),
        class_inv_var.reshape(1, n_cls),
    )
    return sky.reshape(pix), psf.T


def solution(mesh):
    placed = (P(("chan", "vis"), "pix"), P(("chan", "vis")), P("vis"), P("vis"), P(), P("chan"))
    return jax.shard_map(
        functools.partial(shards, mesh.shape["pix"]),
        mesh=mesh,
        in_specs=placed,
        out_specs=(P(("chan", "pix")), P(("chan", "pix"), "vis")),
        check_vma=False,
    )
```
